32 devices in a mesh: dp: 4 (over z), expert: 2 (over x), tensor: 4 (over y, core).
Axes of the slice: x: 2, y: 2, z: 4, core: 2. Of those that a mesh axis runs over, the one named last changes fastest.
Arguments:
- tokens: bfloat16 [256, 4096], P(('dp', 'expert', 'tensor')), may hold values from -6 to 6
- out_grad: bfloat16 [256, 4096], P(('dp', 'expert', 'tensor')), may hold values from -4 to 4
- route_probs: float32 [256, 2], P(('dp', 'expert')), may hold values from 0.2 to 1
- expert_ids: int32 [256, 2], P(('dp', 'expert')), may hold values from 0 to 7, as said below
- slot_index: int32 [256, 2], P(('dp', 'expert')), may hold values from 0 to 10, as said below
- w_gate: bfloat16 [8, 4096, 7168], P('expert', 'dp', 'tensor'), may hold values from -0.09375 to 0.09375
- w_up: bfloat16 [8, 4096, 7168], P('expert', 'dp', 'tensor'), may hold values from -0.09375 to 0.09375
- w_down: bfloat16 [8, 7168, 4096], P('expert', 'tensor', 'dp'), may hold values from -0.0625 to 0.0625
Outputs:
- token_grad: bfloat16 [256, 4096], P(('dp', 'expert', 'tensor'))
- grad_gate: bfloat16 [8, 4096, 7168], P('expert', 'dp', 'tensor')
- grad_up: bfloat16 [8, 4096, 7168], P('expert', 'dp', 'tensor')
- grad_down: bfloat16 [8, 7168, 4096], P('expert', 'tensor', 'dp')
The draws below stay inside these ranges and needn't reach their ends.
Inputs may be any that keep to these rules, and one draw needn't show every extreme that they name: `expert_ids`: the 2 entries of a token are different experts. slot_index[t, k] counts the earlier routes to expert_ids[t, k] within the token's routing block of 32 rows, in order of tokens and then of routes; the value 10 marks a route past the capacity, which is dropped (a count of 10 or more is given as 10). In every draw some expert is filled to 10 slots in every block.
All inputs are finite; a program needn't handle non-finite values.
Results may differ from the reference program's by a relative error of at most 0.011.
Values may be sent and summed in bfloat16 or wider, within the bound.
No kernel may reach another device: no remote copies, remote signals or barrier semaphores. Data moves between devices by JAX's collectives and lax.ppermute only.
A program may use at most 192 MiB of HBM per device.

```python
import jax
import jax.numpy as jnp
from jax import lax

D = 4096
EXPERTS = 8
TOP = 2
FF = 7168
GROUP = 32
CAP = 10
TOKENS = 256


def route_draw(key):
    blocks = TOKENS // GROUP
    base = jax.random.fold_in(key, 7)
    hot_key, pick_key, first_key, second_key = jax.random.split(base, 4)
    hot_expert = jax.random.randint(hot_key, (), 0, EXPERTS)
    pick = jax.random.randint(pick_key, (blocks, GROUP), 0, 2)
    first_any = jax.random.randint(first_key, (blocks, GROUP), 0, EXPERTS)
    first = jnp.where(pick == 1, hot_expert, first_any)
    second = (first + 1 + jax.random.randint(second_key, (blocks, GROUP), 0, EXPERTS - 1)) % EXPERTS
    chosen = jnp.stack([first, second], -1).astype(jnp.int32)
    flat_ids = chosen.reshape(blocks, GROUP * TOP)
    onehot = (flat_ids[:, :, None] == jnp.arange(EXPERTS, dtype=jnp.int32)[None, None, :]).astype(jnp.int32)
    earlier = jnp.cumsum(onehot, axis=1) - onehot
    position = jnp.sum(earlier * onehot, axis=-1)
    position = jnp.minimum(position, CAP).astype(jnp.int32)
    return (chosen.reshape(TOKENS, TOP), position.reshape(TOKENS, TOP))


def draw_expert_ids(key, part):
    return route_draw(key)[0]


def draw_slot_index(key, part):
    return route_draw(key)[1]


def level_of(rng, shape, cuts, low, largest):
    def one(axis_at, blocks):
        steps = jax.random.uniform(jax.random.fold_in(jax.random.fold_in(rng, 6), axis_at), (blocks,), jnp.float32, low / len(cuts), largest / len(cuts))
        return jnp.repeat(jnp.exp(steps), shape[axis_at] // blocks).reshape((-1,) + (1,) * (len(shape) - axis_at - 1))

    gain = one(*cuts[0])
    for cut in cuts[1:]:
        gain = gain * one(*cut)
    return gain


def scatter_about(own_key, extent, spread, most, cuts=(), kind=jnp.bfloat16):
    values = jax.random.normal(own_key, extent, jnp.float32) * spread
    if len(cuts) > 0:
        values = level_of(own_key, extent, cuts, -0.22, 0.18) * values
    return jnp.clip(values, min=-most, max=most).astype(kind)


def setup_inputs(seed: int = 0) -> dict:
    key_of = jax.random.split(jax.random.key(seed), 9)
    return {
        "tokens": scatter_about(key_of[0], (TOKENS, D), 1.0, 6.0, ((0, 32),)),
        "out_grad": scatter_about(key_of[1], (TOKENS, D), 0.5, 4.0, ((0, 32),)),
        "route_probs": jnp.clip(0.2 + 0.8 * jax.random.uniform(key_of[2], (TOKENS, TOP), jnp.float32) ** level_of(key_of[2], (TOKENS, TOP), ((0, 8),), -0.2, 0.2), 0.2, 1.0),
        "expert_ids": draw_expert_ids(jax.random.fold_in(key_of[8], 71), 0),
        "slot_index": draw_slot_index(jax.random.fold_in(key_of[8], 71), 0),
        "w_gate": scatter_about(key_of[5], (EXPERTS, D, FF), D ** -0.5, 0.09375, ((0, 2), (1, 4), (2, 4))),
        "w_up": scatter_about(key_of[6], (EXPERTS, D, FF), D ** -0.5, 0.09375, ((0, 2), (1, 4), (2, 4))),
        "w_down": scatter_about(key_of[7], (EXPERTS, FF, D), FF ** -0.5, 0.0625, ((0, 2), (1, 4), (2, 4))),
    }


def route_tables(expert_ids, slot_index, capacity):
    target = slot_index * EXPERTS + expert_ids
    target = jnp.where(slot_index < capacity, target, -1).astype(jnp.int32)
    places = jnp.arange(capacity * EXPERTS, dtype=jnp.int32)
    return [(places[:, None] == target[None, :, k]).astype(jnp.bfloat16) for k in range(TOP)]


def swiglu_back(pre_gate, pre_up, grad_hidden):
    sigmoid_gate = jax.nn.sigmoid(pre_gate)
    silu_gate = pre_gate * sigmoid_gate
    hidden = (silu_gate * pre_up).astype(jnp.bfloat16)
    up_delta = (grad_hidden * silu_gate).astype(jnp.bfloat16)
    gate_delta = (grad_hidden * pre_up * sigmoid_gate * (1.0 + pre_gate * (1.0 - sigmoid_gate))).astype(jnp.bfloat16)
    return hidden, gate_delta, up_delta


def reference(tokens, out_grad, route_probs, expert_ids, slot_index, w_gate, w_up, w_down):
    blocks = TOKENS // GROUP
    capacity = CAP

    def dispatch(inputs):
        block_x, block_dy, block_probs, block_ids, block_slots = inputs
        tables = route_tables(block_ids, block_slots, capacity)
        table_sum = tables[0] + tables[1]
        x_buf = jnp.dot(table_sum, block_x, preferred_element_type=jnp.float32).astype(jnp.bfloat16)
        grad_buf = jnp.zeros((capacity * EXPERTS, D), jnp.float32)
        for k in range(TOP):
            scaled = (block_probs[:, k:k + 1] * block_dy.astype(jnp.float32)).astype(jnp.bfloat16)
            grad_buf = grad_buf + jnp.dot(tables[k], scaled, preferred_element_type=jnp.float32)
        grad_buf = grad_buf.astype(jnp.bfloat16)
        return (x_buf.reshape(capacity, EXPERTS, D), grad_buf.reshape(capacity, EXPERTS, D),
                table_sum.astype(jnp.float32))

    x_bufs, grad_bufs, table_all = lax.map(dispatch, (
        tokens.reshape(blocks, GROUP, D), out_grad.reshape(blocks, GROUP, D),
        route_probs.reshape(blocks, GROUP, TOP), expert_ids.reshape(blocks, GROUP, TOP),
        slot_index.reshape(blocks, GROUP, TOP)))
    expert_x = jnp.moveaxis(x_bufs, 2, 0).reshape(EXPERTS, blocks * capacity, D)
    expert_g = jnp.moveaxis(grad_bufs, 2, 0).reshape(EXPERTS, blocks * capacity, D)

    def expert_back(inputs):
        rows_x, rows_g, gate_w, up_w, down_w = inputs
        pre_gate = jnp.dot(rows_x, gate_w, preferred_element_type=jnp.float32)
        pre_up = jnp.dot(rows_x, up_w, preferred_element_type=jnp.float32)
        grad_hidden = jnp.dot(rows_g, down_w.T, preferred_element_type=jnp.float32)
        hidden, gate_delta, up_delta = swiglu_back(pre_gate, pre_up, grad_hidden)
        g_down = jnp.dot(hidden.T, rows_g, preferred_element_type=jnp.float32).astype(jnp.bfloat16)
        g_gate = jnp.dot(rows_x.T, gate_delta, preferred_element_type=jnp.float32).astype(jnp.bfloat16)
        g_up = jnp.dot(rows_x.T, up_delta, preferred_element_type=jnp.float32).astype(jnp.bfloat16)
        row_grad = jnp.dot(gate_delta, gate_w.T, preferred_element_type=jnp.float32)
        row_grad = row_grad + jnp.dot(up_delta, up_w.T, preferred_element_type=jnp.float32)
        return g_gate, g_up, g_down, row_grad

    grad_gate, grad_up, grad_down, row_grad = lax.map(expert_back, (expert_x, expert_g, w_gate, w_up, w_down))
    row_grad = row_grad.reshape(EXPERTS, blocks, capacity, D)
    row_grad = jnp.transpose(row_grad, (1, 2, 0, 3)).reshape(blocks, capacity * EXPERTS, D)
    token_grad = jnp.einsum("bjt,bjd->btd", table_all, row_grad, precision=lax.Precision.HIGHEST)
    token_grad = token_grad.reshape(TOKENS, D).astype(jnp.bfloat16)
    return token_grad, grad_gate, grad_up, grad_down
```

```python
import jax
import jax.numpy as jnp
from jax import lax
from jax.sharding import PartitionSpec as P

EXPERTS = 8
TOP = 2
LANES = 128
F32 = jnp.float32
BF16 = jnp.bfloat16


def swiglu_back(pre_gate, pre_up, grad_hidden):
    sigmoid_gate = jax.nn.sigmoid(pre_gate)
    silu_gate = pre_gate * sigmoid_gate
    hidden = (silu_gate * pre_up).astype(BF16)
    up_delta = (grad_hidden * silu_gate).astype(BF16)
    gate_delta = (
        grad_hidden * pre_up * sigmoid_gate * (1.0 + pre_gate * (1.0 - sigmoid_gate))
    ).astype(BF16)
    return (hidden, gate_delta, up_delta)


def strides(n):
    return [1 << k for k in range(n.bit_length() - 1)]


def swap(value, n, stride):
    return lax.ppermute(value, "dp", [(i, i ^ stride) for i in range(n)])


def sum_rows(partial):
    n = lax.axis_size("dp")
    at = lax.axis_index("dp")
    part = partial
    for stride in strides(n):
        half = part.shape[0] // 2
        bit = (at // stride) % 2
        keep = lax.dynamic_slice_in_dim(part, bit * half, half, 0)
        send = lax.dynamic_slice_in_dim(part, (1 - bit) * half, half, 0)
        part = keep.astype(F32) + swap(send.astype(BF16), n, stride).astype(F32)
        if 2 * stride < n:
            part = part.astype(BF16)
    return part


def all_rows(first, others, work):
    n = lax.axis_size("dp")
    at = lax.axis_index("dp")

    def grow(own, stride):
        other = swap(own, n, stride)
        low = (at // stride) % 2 == 0
        whole = jnp.concatenate([jnp.where(low, own, other), jnp.where(low, other, own)], 0)
        return other, whole

    steps = list(reversed(strides(n)))
    arrays = [first] + list(others)
    for k in range(len(arrays)):
        for step, stride in enumerate(steps):
            if k > 1 and step == len(steps) - 1:
                arrays[k], back = lax.optimization_barrier((arrays[k], done[0]))
                done = (back,) + done[1:]
            other, arrays[k] = grow(arrays[k], stride)
            if step == 0 and k + 1 < len(arrays):
                arrays[k + 1], arrays[k] = lax.optimization_barrier((arrays[k + 1], arrays[k]))
        if k == 0:
            done = work(arrays[0])
    return arrays, done


def shards(tokens, out_grad, route_probs, expert_ids, slot_index, w_gate, w_up, w_down):
    dp = lax.axis_size("dp")
    ex = lax.axis_size("expert")
    tn = lax.axis_size("tensor")
    held, model_width = tokens.shape
    block_rows = held * tn
    blocks = dp * ex
    capacity = 5 * block_rows * TOP // (4 * EXPERTS)
    local_experts, slice_width, hidden_width = w_gate.shape
    token_count = blocks * block_rows
    rows = blocks * capacity
    places = local_experts * rows

    mine = lax.axis_index("tensor") * held

    def own_rows(routes):
        return lax.dynamic_slice_in_dim(routes, mine, held, 0)

    pieces, left = [], own_rows(route_probs)
    for _ in range(3):
        piece = lax.reduce_precision(left, 8, 7)
        pieces.append(piece)
        left = left - piece
    info = [own_rows(expert_ids).astype(F32), own_rows(slot_index).astype(F32)] + pieces
    info = jnp.concatenate(info, 1).astype(BF16)
    info = jnp.pad(info, ((0, 0), (0, LANES - info.shape[1])))
    both = jnp.concatenate(
        [
            tokens.reshape(held, dp, slice_width),
            jnp.broadcast_to(info[:, None, :], (held, dp, LANES)),
            out_grad.reshape(held, dp, slice_width),
        ],
        2,
    )
    both = lax.all_to_all(
        jnp.moveaxis(both, 1, 0), "dp", split_axis=0, concat_axis=0, tiled=True
    ).reshape(dp * held, 2 * slice_width + LANES)
    first = lax.all_gather(
        both[:, : slice_width + LANES], ("expert", "tensor"), axis=0, tiled=True
    )
    own_dy = both[:, slice_width + LANES :]
    all_x = first[:, :slice_width]
    info = first[:, slice_width : slice_width + 5 * TOP].astype(F32).reshape(token_count, 5, TOP)
    ids = info[:, 0].astype(jnp.int32).T
    slots = info[:, 1].astype(jnp.int32).T
    probs = ((info[:, 2] + info[:, 3]) + info[:, 4]).T
    block = lax.broadcasted_iota(jnp.int32, (ex, tn, dp, held), 2) * ex
    block = (block + lax.broadcasted_iota(jnp.int32, (ex, tn, dp, held), 0)).reshape(token_count)
    local = ids - lax.axis_index("expert") * local_experts
    kept = (slots < capacity) & (local >= 0) & (local < local_experts)
    target = jnp.where(kept, local * rows + block[None, :] * capacity + slots, -1)
    place = jnp.arange(places, dtype=jnp.int32)
    tables = [(place[:, None] == target[k][None, :]).astype(BF16) for k in range(TOP)]
    table_sum = tables[0] + tables[1]

    x_rows = jnp.dot(table_sum, all_x, preferred_element_type=F32).astype(BF16)
    x_exp = x_rows.reshape(local_experts, rows, slice_width)

    def flat(value):
        return value.astype(BF16).reshape(places, hidden_width)

    def per_expert(value):
        return value.reshape(local_experts, rows, hidden_width)

    part_gate = flat(jnp.einsum("lrd,ldf->lrf", x_exp, w_gate, preferred_element_type=F32))
    own_dy, part_gate = lax.optimization_barrier((own_dy, part_gate))
    pre_gate = sum_rows(part_gate)
    all_dy = lax.all_gather(own_dy, ("expert", "tensor"), axis=0, tiled=True)
    scaled = [(probs[k][:, None] * all_dy.astype(F32)).astype(BF16) for k in range(TOP)]
    g_rows = jnp.dot(
        jnp.concatenate(tables, 1), jnp.concatenate(scaled, 0), preferred_element_type=F32
    ).astype(BF16)
    g_exp = g_rows.reshape(local_experts, rows, slice_width)

    pre_up = sum_rows(flat(jnp.einsum("lrd,ldf->lrf", x_exp, w_up, preferred_element_type=F32)))
    grad_hidden = sum_rows(
        flat(jnp.einsum("lrd,lfd->lrf", g_exp, w_down, preferred_element_type=F32))
    )
    hidden, gate_delta, up_delta = swiglu_back(pre_gate, pre_up, grad_hidden)
    def gate_work(rows_all):
        delta = per_expert(rows_all)
        back = jnp.einsum("lrf,ldf->lrd", delta, w_gate, preferred_element_type=F32)
        grad = jnp.einsum("lrd,lrf->ldf", x_exp, delta, preferred_element_type=F32)
        return back, grad.astype(BF16)

    arrays, (row_grad, grad_gate) = all_rows(gate_delta, (up_delta, hidden), gate_work)
    up_delta, hidden = per_expert(arrays[1]), per_expert(arrays[2])
    up_delta, row_grad = lax.optimization_barrier((up_delta, row_grad))
    row_grad = row_grad + jnp.einsum("lrf,ldf->lrd", up_delta, w_up, preferred_element_type=F32)
    grad_up = jnp.einsum("lrd,lrf->ldf", x_exp, up_delta, preferred_element_type=F32)
    grad_down = jnp.einsum("lrf,lrd->lfd", hidden, g_exp, preferred_element_type=F32)

    token_part = jnp.dot(
        table_sum.astype(F32).T,
        row_grad.reshape(places, slice_width),
        precision=lax.Precision.HIGHEST,
        preferred_element_type=F32,
    )
    parts = lax.all_to_all(
        token_part.astype(BF16).reshape(ex * tn, dp * held, slice_width),
        ("expert", "tensor"),
        split_axis=0,
        concat_axis=0,
        tiled=True,
    )
    token_grad = jnp.sum(parts.astype(F32), 0).astype(BF16)
    token_grad = lax.all_to_all(
        token_grad.reshape(dp, held, slice_width), "dp", split_axis=0, concat_axis=0, tiled=True
    )
    token_grad = jnp.moveaxis(token_grad, 0, 1).reshape(held, model_width)
    return (token_grad, grad_gate, grad_up.astype(BF16), grad_down.astype(BF16))


def solution(mesh):
    rows = P(("dp", "expert", "tensor"), None)
    routes = P(("dp", "expert"), None)
    wide = P("expert", "dp", "tensor")
    tall = P("expert", "tensor", "dp")
    return jax.shard_map(
        shards,
        mesh=mesh,
        in_specs=(rows, rows, routes, routes, routes, wide, wide, tall),
        out_specs=(rows, wide, wide, tall),
        check_vma=False,
    )
```
